64 devices in a mesh: rep: 4 (over x, y), data: 16 (over z, core).
Axes of the slice: x: 2, y: 2, z: 8, core: 2. Of those that a mesh axis runs over, the one named last changes fastest.
The devices are a block of a 4x4x8 slice.
Arguments:
- x: bfloat16 [8192, 4096], P(('rep', 'data')), parts along dimension 0
- adapter_id: int32 [8192], P(('rep', 'data')), parts along dimension 0
- dout: bfloat16 [8192, 4096], P(('rep', 'data')), parts along dimension 0
- w_gate: bfloat16 [4096, 14336], replicated
- w_up: bfloat16 [4096, 14336], replicated
- w_down: bfloat16 [14336, 4096], replicated
- a_gate: bfloat16 [32, 4096, 16], P('data')
- b_gate: bfloat16 [32, 16, 14336], P('data')
- a_up: bfloat16 [32, 4096, 16], P('data')
- b_up: bfloat16 [32, 16, 14336], P('data')
- a_down: bfloat16 [32, 14336, 16], P('data')
- b_down: bfloat16 [32, 16, 4096], P('data')
Outputs:
- output 1: bfloat16 [8192, 4096], P(('rep', 'data')), parts along dimension 0
- output 2: bfloat16 [8192, 4096], P(('rep', 'data')), parts along dimension 0
- output 3: float32 [128, 4096, 16], P(('rep', 'data')), parts along dimension 0
- output 4: float32 [128, 16, 14336], P(('rep', 'data')), parts along dimension 0
- output 5: float32 [128, 4096, 16], P(('rep', 'data')), parts along dimension 0
- output 6: float32 [128, 16, 14336], P(('rep', 'data')), parts along dimension 0
- output 7: float32 [128, 14336, 16], P(('rep', 'data')), parts along dimension 0
- output 8: float32 [128, 16, 4096], P(('rep', 'data')), parts along dimension 0
There are 4 independent parts. The reference program is written for one: setup_inputs(seed, part) draws one part's arguments, and reference() takes and returns one part's arrays. A program takes and returns all parts, laid end to end along the dimension named above; an argument that names none is the same for every part.
All inputs are finite; a program needn't handle non-finite values.
Results may differ from the reference program's by a relative error of at most 0.00124.
Values are sent between devices in bfloat16 or wider.
A program may use at most 768 MiB of HBM per device.

```python
import jax
import jax.numpy as jnp
from jax import lax

TOKENS = 128
ADAPTERS = 2
MODEL_DIM = 4096
HIDDEN_DIM = 14336
LORA_RANK = 16
GROUP_SIZE = 16
CAPACITY = 24
LORA_ALPHA = 32
BLOCK_ROWS = 32

PART_TOKENS = TOKENS * GROUP_SIZE
NUM_ADAPTERS = ADAPTERS * GROUP_SIZE
LORA_SCALE = LORA_ALPHA / LORA_RANK


def draw_ids(rand_key):
    key_hot, key_off, key_shift, key_perm = jax.random.split(rand_key, 4)
    hot_owner = jax.random.randint(key_hot, (), 0, GROUP_SIZE)
    start_offset = jax.random.randint(key_off, (), 0, GROUP_SIZE - 1)
    owner_shift = jax.random.randint(key_shift, (GROUP_SIZE,), 0, ADAPTERS)
    spare_rows = TOKENS - CAPACITY
    source_dev = jnp.arange(GROUP_SIZE)[:, None]
    column_idx = jnp.arange(TOKENS)[None, :]
    hot_mask = column_idx < CAPACITY
    hot_local = (source_dev * CAPACITY + column_idx + owner_shift[hot_owner]) % ADAPTERS
    flat_index = start_offset + source_dev * spare_rows + column_idx - CAPACITY
    other_owner = (hot_owner + 1 + flat_index % (GROUP_SIZE - 1)) % GROUP_SIZE
    visit_count = flat_index // (GROUP_SIZE - 1)
    other_local = (visit_count + owner_shift[other_owner]) % ADAPTERS
    owner_ids = jnp.where(hot_mask, hot_owner, other_owner)
    local_ids = jnp.where(hot_mask, hot_local, other_local)
    id_table = owner_ids * ADAPTERS + local_ids
    perm_keys = jax.random.split(key_perm, GROUP_SIZE)
    perm_rows = jax.vmap(lambda perm_key: jax.random.permutation(perm_key, TOKENS))(perm_keys)
    id_table = jnp.take_along_axis(id_table, perm_rows, axis=1)
    return id_table.reshape(-1).astype(jnp.int32)


def normal_bf16(key_one, arr_shape, spread):
    return (jax.random.normal(key_one, arr_shape, jnp.float32) * spread).astype(jnp.bfloat16)


def setup_inputs(seed: int = 0, part: int = 0) -> dict:
    base_key = jax.random.key(seed)
    part_key = jax.random.fold_in(base_key, part)
    shared_keys = jax.random.split(base_key, 9)
    part_keys = jax.random.split(part_key, 3)
    b_std = 0.3 * LORA_RANK ** -0.5 / LORA_SCALE
    d_std = MODEL_DIM ** -0.5
    f_std = HIDDEN_DIM ** -0.5
    return {
        'x': normal_bf16(part_keys[0], (PART_TOKENS, MODEL_DIM), 1.0),
        'adapter_id': draw_ids(part_keys[1]),
        'dout': normal_bf16(part_keys[2], (PART_TOKENS, MODEL_DIM), 1.0),
        'w_gate': normal_bf16(shared_keys[0], (MODEL_DIM, HIDDEN_DIM), d_std),
        'w_up': normal_bf16(shared_keys[1], (MODEL_DIM, HIDDEN_DIM), d_std),
        'w_down': normal_bf16(shared_keys[2], (HIDDEN_DIM, MODEL_DIM), f_std),
        'a_gate': normal_bf16(shared_keys[3], (NUM_ADAPTERS, MODEL_DIM, LORA_RANK), d_std),
        'b_gate': normal_bf16(shared_keys[4], (NUM_ADAPTERS, LORA_RANK, HIDDEN_DIM), b_std),
        'a_up': normal_bf16(shared_keys[5], (NUM_ADAPTERS, MODEL_DIM, LORA_RANK), d_std),
        'b_up': normal_bf16(shared_keys[6], (NUM_ADAPTERS, LORA_RANK, HIDDEN_DIM), b_std),
        'a_down': normal_bf16(shared_keys[7], (NUM_ADAPTERS, HIDDEN_DIM, LORA_RANK), f_std),
        'b_down': normal_bf16(shared_keys[8], (NUM_ADAPTERS, LORA_RANK, MODEL_DIM), b_std),
    }


def bf16_cast(values):
    return values.astype(jnp.bfloat16).astype(jnp.float32)


def reference(x, adapter_id, dout, w_gate, w_up, w_down, a_gate, b_gate, a_up, b_up, a_down, b_down):
    gate_wt = w_gate.astype(jnp.float32)
    up_wt = w_up.astype(jnp.float32)
    down_wt = w_down.astype(jnp.float32)
    model_width = x.shape[1]
    num_blocks = x.shape[0] // BLOCK_ROWS

    def block_step(grad_sums, block_in):
        x_blk, id_blk, dy_blk = block_in
        x_rows = x_blk.astype(jnp.float32)
        dy_rows = dy_blk.astype(jnp.float32)
        ag_rows = a_gate[id_blk].astype(jnp.float32)
        bg_rows = b_gate[id_blk].astype(jnp.float32)
        au_rows = a_up[id_blk].astype(jnp.float32)
        bu_rows = b_up[id_blk].astype(jnp.float32)
        ad_rows = a_down[id_blk].astype(jnp.float32)
        bd_rows = b_down[id_blk].astype(jnp.float32)
        p_gate = bf16_cast(jnp.einsum('td,tdr->tr', x_rows, ag_rows))
        p_up = bf16_cast(jnp.einsum('td,tdr->tr', x_rows, au_rows))
        e_gate = bf16_cast(LORA_SCALE * jnp.einsum('tr,trf->tf', p_gate, bg_rows))
        e_up = bf16_cast(LORA_SCALE * jnp.einsum('tr,trf->tf', p_up, bu_rows))
        gate_pre = jnp.dot(x_rows, gate_wt) + e_gate
        up_pre = jnp.dot(x_rows, up_wt) + e_up
        gate_sig = jax.nn.sigmoid(gate_pre)
        gate_act = gate_pre * gate_sig
        hidden = bf16_cast(gate_act * up_pre)
        p_down = bf16_cast(jnp.einsum('tf,tfr->tr', hidden, ad_rows))
        e_down = bf16_cast(LORA_SCALE * jnp.einsum('tr,trd->td', p_down, bd_rows))
        out_blk = (x_rows + jnp.dot(hidden, down_wt) + e_down).astype(jnp.bfloat16)
        q_down = bf16_cast(LORA_SCALE * jnp.einsum('td,trd->tr', dy_rows, bd_rows))
        dh_lora = bf16_cast(jnp.einsum('tr,tfr->tf', q_down, ad_rows))
        d_hidden = jnp.einsum('td,fd->tf', dy_rows, down_wt) + dh_lora
        d_gate = bf16_cast(d_hidden * up_pre * gate_sig * (1.0 + gate_pre * (1.0 - gate_sig)))
        d_up = bf16_cast(d_hidden * gate_act)
        q_gate = bf16_cast(LORA_SCALE * jnp.einsum('tf,trf->tr', d_gate, bg_rows))
        q_up = bf16_cast(LORA_SCALE * jnp.einsum('tf,trf->tr', d_up, bu_rows))
        dx_lora = bf16_cast(jnp.einsum('tr,tdr->td', q_gate, ag_rows) + jnp.einsum('tr,tdr->td', q_up, au_rows))
        dx_blk = (dy_rows + jnp.einsum('tf,df->td', d_gate, gate_wt) + jnp.einsum('tf,df->td', d_up, up_wt) + dx_lora).astype(jnp.bfloat16)
        updates = (
            jnp.einsum('td,tr->tdr', x_rows, q_gate),
            LORA_SCALE * jnp.einsum('tr,tf->trf', p_gate, d_gate),
            jnp.einsum('td,tr->tdr', x_rows, q_up),
            LORA_SCALE * jnp.einsum('tr,tf->trf', p_up, d_up),
            jnp.einsum('tf,tr->tfr', hidden, q_down),
            LORA_SCALE * jnp.einsum('tr,td->trd', p_down, dy_rows),
        )
        new_sums = tuple(grad_acc.at[id_blk].add(grad_upd) for grad_acc, grad_upd in zip(grad_sums, updates))
        return new_sums, (out_blk, dx_blk)

    init_sums = tuple(jnp.zeros(weight.shape, jnp.float32) for weight in (a_gate, b_gate, a_up, b_up, a_down, b_down))
    blocks_in = (
        x.reshape(num_blocks, BLOCK_ROWS, model_width),
        adapter_id.reshape(num_blocks, BLOCK_ROWS),
        dout.reshape(num_blocks, BLOCK_ROWS, model_width),
    )
    grad_sums, (out_rows, dx_rows) = lax.scan(block_step, init_sums, blocks_in)
    return (out_rows.reshape(-1, model_width), dx_rows.reshape(-1, model_width), grad_sums[0], grad_sums[1], grad_sums[2], grad_sums[3], grad_sums[4], grad_sums[5])
```

```python
import functools

import jax
import jax.numpy as jnp
from jax import lax
from jax.experimental import pallas as pl
from jax.experimental.pallas import tpu as pltpu
from jax.sharding import PartitionSpec as P

LORA_ALPHA = 32
LANES = 128
TILE = 512
CHUNK = 1024
F32 = jnp.float32
BF16 = jnp.bfloat16


def nn(a, b):
    return lax.dot_general(a, b, (((1,), (0,)), ((), ())), preferred_element_type=F32)


def nt(a, b):
    return lax.dot_general(a, b, (((1,), (1,)), ((), ())), preferred_element_type=F32)


def tn(a, b):
    return lax.dot_general(a, b, (((0,), (0,)), ((), ())), preferred_element_type=F32)


def rounded(v):
    return v.astype(BF16).astype(F32)


def layer_kernel(
    scale, sizes,
    n_ref, xr_ref, dr_ref, pack_ref, spread_ref,
    ag0, ag1, au0, au1, bd0, bd1,
    wg_ref, wu_ref, wd_ref, bg0, bg1, bu0, bu1, ad0, ad1,
    out_ref, dx_ref,
    gag0, gag1, gau0, gau1, gbd0, gbd1, gbg0, gbg1, gbu0, gbu1, gad0, gad1,
    xbuf, dbuf, xs, ds, mask_s, oacc, dacc, pg_s, pu_s, qd_s, pgt_s, put_s, qdt_s, pd_s, qg_s, qu_s, sems,
):
    i = pl.program_id(0)
    last = pl.num_programs(0) - 1
    n = n_ref[0]
    width = xs.shape[1]
    half = ag0.shape[0]

    def both(a, b, c=slice(None)):
        return jnp.concatenate([a[:, c], b[:, c]], axis=0)

    def store(a, b, v, c=slice(None)):
        a[:, c] = v[:half]
        b[:, c] = v[half:]

    @pl.when(i == 0)
    def _():
        load_x = pltpu.make_async_copy(xr_ref, xbuf, sems.at[0])
        load_d = pltpu.make_async_copy(dr_ref, dbuf, sems.at[1])
        load_x.start()
        load_d.start()
        load_x.wait()
        load_d.wait()

    def start(m):
        take = pack_ref[:m, :]
        for j in range(0, width, CHUNK):
            e = slice(j, j + CHUNK)
            xs[:m, e] = nn(take, xbuf[:, e]).astype(BF16)
            ds[:m, e] = nn(take, dbuf[:, e]).astype(BF16)
        mask_s[:m, :] = nn(take, xbuf[:, width:])[:, : 2 * half]
        keep = mask_s[:m, :] > 0

        def masked(v):
            return jnp.where(keep, v, 0.0)

        x = xs[:m, :]
        pg = masked(nt(x, both(ag0, ag1)))
        pu = masked(nt(x, both(au0, au1)))
        qd = masked(scale * nt(ds[:m, :], both(bd0, bd1)))
        for v, s, t in ((pg, pg_s, pgt_s), (pu, pu_s, put_s), (qd, qd_s, qdt_s)):
            s[:m, :] = v.astype(BF16)
            t[:, :m] = v.T.astype(BF16)
        oacc[:m, :] = jnp.zeros((m, width), F32)
        dacc[:m, :] = jnp.zeros((m, width), F32)
        for s in (pd_s, qg_s, qu_s):
            s[:m, :] = jnp.zeros((m, 2 * half), F32)

    def step(m):
        x = xs[:m, :]
        bg, bu, ad = both(bg0, bg1), both(bu0, bu1), both(ad0, ad1)
        g = nn(x, wg_ref[...]) + rounded(scale * nn(pg_s[:m, :], bg))
        u = nn(x, wu_ref[...]) + rounded(scale * nn(pu_s[:m, :], bu))
        dh = nt(ds[:m, :], wd_ref[...]) + rounded(nn(qd_s[:m, :], ad))
        sig = jax.nn.sigmoid(g)
        act = g * sig
        h = (act * u).astype(BF16)
        dg = (dh * u * sig * (1.0 + g * (1.0 - sig))).astype(BF16)
        du = (dh * act).astype(BF16)
        for j in range(0, width, CHUNK):
            e = slice(j, j + CHUNK)
            oacc[:m, e] += nn(h, wd_ref[:, e])
            dacc[:m, e] += nt(dg, wg_ref[e, :]) + nt(du, wu_ref[e, :])
        pd_s[:m, :] += nt(h, ad)
        qg_s[:m, :] += nt(dg, bg)
        qu_s[:m, :] += nt(du, bu)
        store(gbg0, gbg1, scale * nn(pgt_s[:, :m], dg))
        store(gbu0, gbu1, scale * nn(put_s[:, :m], du))
        store(gad0, gad1, nn(qdt_s[:, :m], h))

    def finish(m):
        keep = mask_s[:m, :] > 0
        pd = jnp.where(keep, pd_s[:m, :], 0.0)
        qg = jnp.where(keep, scale * qg_s[:m, :], 0.0)
        qu = jnp.where(keep, scale * qu_s[:m, :], 0.0)
        pdb, qgb, qub = pd.astype(BF16), qg.astype(BF16), qu.astype(BF16)
        pdt, qgt, qut = pd.T.astype(BF16), qg.T.astype(BF16), qu.T.astype(BF16)
        put = spread_ref[:, :m]
        for j in range(0, width, CHUNK):
            e = slice(j, j + CHUNK)
            x = xs[:m, e]
            d = ds[:m, e]
            out = (x.astype(F32) + oacc[:m, e] + rounded(scale * nn(pdb, both(bd0, bd1, e)))).astype(BF16)
            dx = d.astype(F32) + dacc[:m, e] + rounded(nn(qgb, both(ag0, ag1, e)) + nn(qub, both(au0, au1, e)))
            xbuf[:, e] = nn(put, out).astype(BF16)
            dbuf[:, e] = nn(put, dx.astype(BF16)).astype(BF16)
            store(gag0, gag1, nn(qgt, x), e)
            store(gau0, gau1, nn(qut, x), e)
            store(gbd0, gbd1, scale * nn(pdt, d), e)

    lo = 0
    for m in sizes:
        fits = n <= m if lo == 0 else (n > lo) & (n <= m)
        lo = m

        @pl.when(fits & (i == 0))
        def _(m=m):
            start(m)

        @pl.when(fits)
        def _(m=m):
            step(m)

        @pl.when(fits & (i == last))
        def _(m=m):
            finish(m)

    @pl.when(i == last)
    def _():
        save_x = pltpu.make_async_copy(xbuf.at[:, pl.ds(0, width)], out_ref, sems.at[0])
        save_d = pltpu.make_async_copy(dbuf, dx_ref, sems.at[1])
        save_x.start()
        save_d.start()
        save_x.wait()
        save_d.wait()


def layer(scale, sizes, n, xr, dr, pack, spread, ag, au, bd, wg, wu, wd, bg, bu, ad):
    rows, width = dr.shape
    hidden = wg.shape[1]
    half = ag[0].shape[0]
    k = 2 * half
    once = pl.Buffered(1)

    def fixed(i, n):
        return (0, 0)

    def col(i, n):
        return (0, i)

    def row(i, n):
        return (i, 0)

    def whole(shape):
        return pl.BlockSpec(shape, fixed, pipeline_mode=once)

    hbm = pl.BlockSpec(memory_space=pl.ANY)
    strip = pl.BlockSpec((half, TILE), col)
    square = whole((rows, rows))
    wide = whole((half, width))
    grid_spec = pltpu.PrefetchScalarGridSpec(
        num_scalar_prefetch=1,
        grid=(hidden // TILE,),
        in_specs=[hbm, hbm, square, square] + [wide] * 6
        + [pl.BlockSpec((width, TILE), col), pl.BlockSpec((width, TILE), col), pl.BlockSpec((TILE, width), row)]
        + [strip] * 6,
        out_specs=[hbm, hbm] + [wide] * 6 + [strip] * 6,
        scratch_shapes=[pltpu.VMEM(xr.shape, BF16), pltpu.VMEM((rows, width), BF16)]
        + [pltpu.VMEM((rows, width), BF16)] * 2 + [pltpu.VMEM((rows, k), F32)]
        + [pltpu.VMEM((rows, width), F32)] * 2 + [pltpu.VMEM((rows, k), BF16)] * 3
        + [pltpu.VMEM((k, rows), BF16)] * 3 + [pltpu.VMEM((rows, k), F32)] * 3 + [pltpu.SemaphoreType.DMA((2,))],
    )
    shape = jax.ShapeDtypeStruct
    return pl.pallas_call(
        functools.partial(layer_kernel, scale, sizes),
        grid_spec=grid_spec,
        out_shape=[shape((rows, width), BF16)] * 2 + [shape((half, width), F32)] * 6 + [shape((half, hidden), F32)] * 6,
        compiler_params=pltpu.CompilerParams(dimension_semantics=("arbitrary",), vmem_limit_bytes=63_000_000),
        cost_estimate=pl.CostEstimate(flops=12 * sizes[0] * width * hidden, bytes_accessed=6 * width * hidden, transcendentals=0),
    )(n, xr, dr, pack, spread, *ag, *au, *bd, wg, wu, wd, *bg, *bu, *ad)


def solution(mesh):
    group = mesh.shape['data']
    tok = P(('rep', 'data'), None)
    ids_spec = P(('rep', 'data'))
    full = P(None, None)
    own = P('data', None, None)
    grad = P(('rep', 'data'), None, None)
    swap = [(i, i ^ 1) for i in range(group)]

    def device_fn(x, ids, dy, w_gate, w_up, w_down, a_gate, b_gate, a_up, b_up, a_down, b_down):
        tokens, width = x.shape
        n_local, _, rank = a_gate.shape
        scale = LORA_ALPHA / rank
        cap = ((3 * tokens + 8 * group - 1) // (8 * group)) * 8
        slots = group * cap
        part = cap // 2
        half = n_local * rank
        iota = functools.partial(lax.broadcasted_iota, jnp.int32)

        owner = ids // n_local
        earlier = iota((tokens, tokens), 0) > iota((tokens, tokens), 1)
        order = jnp.sum(jnp.where(earlier & (owner[:, None] == owner[None, :]), 1, 0), axis=1)
        core = (order + owner // 2 + lax.axis_index('data')) % 2
        dest = ((owner // 2) * 2 + core) * cap + (owner % 2) * part + order // 2
        send = (iota((slots, tokens), 0) == dest[None, :]).astype(BF16)
        column = iota((tokens, LANES), 1)
        first = ((owner % 2) ^ core) * half + (ids % n_local) * rank
        flags = ((column >= first[:, None]) & (column < first[:, None] + rank)).astype(BF16)

        def exchange(rows):
            return lax.all_to_all(rows, 'data', 0, 0, tiled=True)

        xr = exchange(nn(send, jnp.concatenate([x, flags], axis=1)).astype(BF16))
        dr = exchange(nn(send, dy).astype(BF16))

        valid = jnp.sum(xr[:, width:].astype(F32), axis=1) > 0
        upto = (iota((slots, slots), 0) >= iota((slots, slots), 1)) & valid[None, :]
        place = jnp.where(valid, jnp.sum(jnp.where(upto, 1, 0), axis=1) - 1, -1)
        count = jnp.sum(jnp.where(valid, 1, 0)).astype(jnp.int32).reshape(1)
        pack = (place[None, :] == iota((slots, slots), 0)).astype(BF16)
        spread = (place[:, None] == iota((slots, slots), 1)).astype(BF16)

        def flat_a(a):
            v = jnp.swapaxes(a, 1, 2).reshape(half, a.shape[1])
            return v, lax.ppermute(v, 'data', swap)

        def flat_b(b):
            v = b.reshape(half, b.shape[2])
            return v, lax.ppermute(v, 'data', swap)

        ag, au, ad = flat_a(a_gate), flat_a(a_up), flat_a(a_down)
        bg, bu, bd = flat_b(b_gate), flat_b(b_up), flat_b(b_down)
        res = layer(scale, (256, 384), count, xr, dr, pack, spread, ag, au, bd, w_gate, w_up, w_down, bg, bu, ad)
        out, dx = [tn(send, exchange(v)).astype(BF16) for v in res[:2]]
        gag, gau, gbd, gbg, gbu, gad = [res[j] + lax.ppermute(res[j + 1], 'data', swap) for j in range(2, 14, 2)]

        def shape_a(v):
            return jnp.swapaxes(v.reshape(n_local, rank, v.shape[1]), 1, 2)

        def shape_b(v):
            return v.reshape(n_local, rank, v.shape[1])

        return out, dx, shape_a(gag), shape_b(gbg), shape_a(gau), shape_b(gbu), shape_a(gad), shape_b(gbd)

    return jax.shard_map(
        device_fn,
        mesh=mesh,
        in_specs=(tok, ids_spec, tok, full, full, full, own, own, own, own, own, own),
        out_specs=(tok, tok, grad, grad, grad, grad, grad, grad),
        check_vma=False,
    )
```

```python
import functools

import jax
import jax.numpy as jnp
from jax import lax
from jax.experimental import pallas as pl
from jax.experimental.pallas import tpu as pltpu
from jax.sharding import PartitionSpec as P


LORA_ALPHA = 32
LANES = 128
CHUNK = 1024
LO = 256
F32 = jnp.float32
BF16 = jnp.bfloat16
Shape = jax.ShapeDtypeStruct
HBM = pl.BlockSpec(memory_space=pl.ANY)


def nn(a, b):
    return lax.dot_general(a, b, (((1,), (0,)), ((), ())), preferred_element_type=F32)


def nt(a, b):
    return lax.dot_general(a, b, (((1,), (1,)), ((), ())), preferred_element_type=F32)


def tn(a, b):
    return lax.dot_general(a, b, (((0,), (0,)), ((), ())), preferred_element_type=F32)


def rounded(v):
    return v.astype(BF16).astype(F32)


def both(a, b, c=slice(None)):
    return jnp.concatenate([a[:, c], b[:, c]], axis=0)


def update_both(a, b, v, block, c=slice(None)):
    half = a.shape[0]
    update(a, c, v[:half], block)
    update(b, c, v[half:], block)


def pieces(width, size):
    return [slice(j, j + size) for j in range(0, width, size)]


def row_blocks(n, rows, body, when=None):
    ok = n >= 0 if when is None else when
    pl.when(ok)(functools.partial(body, slice(0, LO), 0))
    pl.when(ok & (n > LO))(functools.partial(body, slice(LO, rows), 1))


def update(ref, c, v, block):
    ref[:, c] = v if block == 0 else ref[:, c] + v


def at_col(ref, tile):
    return lambda t: ref.at[:, pl.ds(pl.multiple_of(t * tile, tile), tile)]


def at_row(ref, tile):
    return lambda t: ref.at[pl.ds(pl.multiple_of(t * tile, tile), tile), :]


def ring(i, steps, items, sems):
    depth = items[0][1].shape[0]

    def copy(t, s, which):
        src, buf = items[which]
        return pltpu.make_async_copy(src(t), buf.at[s], sems.at[which, s])

    @pl.when(i == 0)
    def _():
        for t in range(depth - 1):
            for which in range(len(items)):
                copy(t, t, which).start()

    ahead = i + depth - 1

    @pl.when(ahead < steps)
    def _():
        for which in range(len(items)):
            copy(ahead, lax.rem(ahead, depth), which).start()

    slot = lax.rem(i, depth)
    for which in range(len(items)):
        copy(i, slot, which).wait()
    return [buf.at[slot] for _, buf in items]


def whole(shape):
    return pl.BlockSpec(shape, lambda i, n: (0, 0), pipeline_mode=pl.Buffered(1))


def col(rows, tile):
    return pl.BlockSpec((rows, tile), lambda i, n: (0, i))


def rows_pair(rows, tile):
    upper = pl.BlockSpec((rows - LO, tile), lambda i, n: (0, jnp.where(n[0] > LO, i, 0)))
    return [col(LO, tile), upper]


def pair_shape(rows, width, dtype):
    return [Shape((LO, width), dtype), Shape((rows - LO, width), dtype)]


def call(body, n, steps, args, in_specs, out_shape, out_specs, scratch, products, weight_bytes):
    return pl.pallas_call(
        body,
        grid_spec=pltpu.PrefetchScalarGridSpec(
            num_scalar_prefetch=1, grid=(steps,), in_specs=in_specs, out_specs=out_specs, scratch_shapes=scratch
        ),
        out_shape=out_shape,
        compiler_params=pltpu.CompilerParams(dimension_semantics=('arbitrary',), vmem_limit_bytes=63_000_000),
        cost_estimate=pl.CostEstimate(flops=LO * weight_bytes * products, bytes_accessed=weight_bytes, transcendentals=0),
    )(n, *args)


def fwd_kernel(
    scale, n_ref, xr_ref, pack_ref, spread_ref, ag0, ag1, au0, au1, bd0, bd1, wg_hbm, wu_hbm, wd_hbm, bg0, bg1, bu0, bu1, ad0, ad1,
    out_ref, xs, mask_ref, pgt_ref, put_ref, pdt_ref, g_lo, g_hi, u_lo, u_hi,
    xbuf, oacc, pg_s, pu_s, pd_s, wgb, wub, wdb, wsem, sem,
):
    i = pl.program_id(0)
    last = pl.num_programs(0) - 1
    n = n_ref[0]
    rows, width = xs.shape
    k = pg_s.shape[1]

    @pl.when(i == 0)
    def _():
        pltpu.make_async_copy(xr_ref, xbuf, sem).start()

    tile = wgb.shape[2]
    weights = [(at_col(wg_hbm, tile), wgb), (at_col(wu_hbm, tile), wub), (at_row(wd_hbm, tile), wdb)]
    wg, wu, wd = ring(i, last + 1, weights, wsem)

    @pl.when(i == 0)
    def _():
        pltpu.make_async_copy(xr_ref, xbuf, sem).wait()

    def start(r, block):
        take = pack_ref[r, :]
        for e in pieces(width, CHUNK):
            xs[r, e] = nn(take, xbuf[:, e]).astype(BF16)
        mask_ref[r, :] = nn(take, xbuf[:, width:])[:, :k]
        keep = mask_ref[r, :] > 0
        x = xs[r, :]
        for a, b, s, t in ((ag0, ag1, pg_s, pgt_ref), (au0, au1, pu_s, put_ref)):
            p = jnp.where(keep, nt(x, both(a, b)), 0.0)
            s[r, :] = p.astype(BF16)
            t[:, r] = p.T.astype(BF16)
        oacc[r, :] = jnp.zeros(x.shape, F32)
        pd_s[r, :] = jnp.zeros(keep.shape, F32)

    def step(r, block):
        x = xs[r, :]
        g = nn(x, wg[...]) + rounded(scale * nn(pg_s[r, :], both(bg0, bg1)))
        u = nn(x, wu[...]) + rounded(scale * nn(pu_s[r, :], both(bu0, bu1)))
        (g_lo, g_hi)[block][...] = g
        (u_lo, u_hi)[block][...] = u
        h = (g * jax.nn.sigmoid(g) * u).astype(BF16)
        for e in pieces(width, CHUNK):
            oacc[r, e] += nn(h, wd[:, e])
        pd_s[r, :] += nt(h, both(ad0, ad1))

    def finish(r, block):
        pd = jnp.where(mask_ref[r, :] > 0, pd_s[r, :], 0.0)
        pdt_ref[:, r] = pd.T.astype(BF16)
        pdb = pd.astype(BF16)
        spread = spread_ref[:, r]
        for e in pieces(width, CHUNK):
            out = xs[r, e].astype(F32) + oacc[r, e] + rounded(scale * nn(pdb, both(bd0, bd1, e)))
            update(xbuf, e, nn(spread, out.astype(BF16)).astype(BF16), block)

    row_blocks(n, rows, start, i == 0)
    row_blocks(n, rows, step)
    row_blocks(n, rows, finish, i == last)

    @pl.when(i == last)
    def _():
        save = pltpu.make_async_copy(xbuf.at[:, pl.ds(0, width)], out_ref, sem)
        save.start()
        save.wait()


def fwd(scale, n, xr, pack, spread, ag, au, bd, wg, wu, wd, bg, bu, ad, tile=512, depth=3):
    rows = xr.shape[0]
    width, hidden = wg.shape
    half = ag[0].shape[0]
    k = 2 * half
    return call(
        functools.partial(fwd_kernel, scale), n, hidden // tile,
        (xr, pack, spread, *ag, *au, *bd, wg, wu, wd, *bg, *bu, *ad),
        [HBM] + [whole((rows, rows))] * 2 + [whole((half, width))] * 6 + [HBM] * 3 + [col(half, tile)] * 6,
        [Shape((rows, width), BF16)] * 2 + [Shape((rows, k), F32)] + [Shape((k, rows), BF16)] * 3 + pair_shape(rows, hidden, F32) * 2,
        [HBM, whole((rows, width)), whole((rows, k))] + [whole((k, rows))] * 3 + rows_pair(rows, tile) * 2,
        [pltpu.VMEM(xr.shape, BF16), pltpu.VMEM((rows, width), F32)] + [pltpu.VMEM((rows, k), BF16)] * 2 + [pltpu.VMEM((rows, k), F32)]
        + [pltpu.VMEM((depth, width, tile), BF16)] * 2 + [pltpu.VMEM((depth, tile, width), BF16)]
        + [pltpu.SemaphoreType.DMA((3, depth)), pltpu.SemaphoreType.DMA],
        1, 6 * width * hidden,
    )


def bwd_kernel(
    scale, n_ref, dr_ref, pack_ref, xs_ref, mask_ref, pgt_ref, put_ref, pdt_ref, bd0, bd1,
    wd_hbm, g_lo, g_hi, u_lo, u_hi, bg0, bg1, bu0, bu1, ad0, ad1,
    ds, qg_ref, qu_ref, gag0, gag1, gau0, gau1, gbd0, gbd1, dg_lo, dg_hi, du_lo, du_hi, gbg0, gbg1, gbu0, gbu1, gad0, gad1,
    dbuf, qd_s, qdt_s, qg_s, qu_s, wdb, wsem, sem,
):
    i = pl.program_id(0)
    last = pl.num_programs(0) - 1
    n = n_ref[0]
    rows, width = ds.shape

    @pl.when(i == 0)
    def _():
        pltpu.make_async_copy(dr_ref, dbuf, sem).start()

    wd, = ring(i, last + 1, [(at_row(wd_hbm, wdb.shape[1]), wdb)], wsem)

    @pl.when(i == 0)
    def _():
        pltpu.make_async_copy(dr_ref, dbuf, sem).wait()

    def start(r, block):
        take = pack_ref[r, :]
        for e in pieces(width, CHUNK):
            ds[r, e] = nn(take, dbuf[:, e]).astype(BF16)
        qd = jnp.where(mask_ref[r, :] > 0, scale * nt(ds[r, :], both(bd0, bd1)), 0.0)
        qd_s[r, :] = qd.astype(BF16)
        qdt_s[:, r] = qd.T.astype(BF16)
        for s in (qg_s, qu_s):
            s[r, :] = jnp.zeros(qd.shape, F32)

    def step(r, block):
        for c in pieces(wd.shape[0], CHUNK // 2):
            bg, bu, ad = both(bg0, bg1, c), both(bu0, bu1, c), both(ad0, ad1, c)
            dh = nt(ds[r, :], wd[c, :]) + rounded(nn(qd_s[r, :], ad))
            g = (g_lo, g_hi)[block][:, c]
            u = (u_lo, u_hi)[block][:, c]
            sig = jax.nn.sigmoid(g)
            act = g * sig
            h = (act * u).astype(BF16)
            dg = (dh * u * sig * (1.0 + g * (1.0 - sig))).astype(BF16)
            du = (dh * act).astype(BF16)
            (dg_lo, dg_hi)[block][:, c] = dg
            (du_lo, du_hi)[block][:, c] = du
            qg_s[r, :] += nt(dg, bg)
            qu_s[r, :] += nt(du, bu)
            update_both(gbg0, gbg1, scale * nn(pgt_ref[:, r], dg), block, c)
            update_both(gbu0, gbu1, scale * nn(put_ref[:, r], du), block, c)
            update_both(gad0, gad1, nn(qdt_s[:, r], h), block, c)

    def finish(r, block):
        keep = mask_ref[r, :] > 0
        qg = jnp.where(keep, scale * qg_s[r, :], 0.0)
        qu = jnp.where(keep, scale * qu_s[r, :], 0.0)
        qg_ref[r, :] = qg.astype(BF16)
        qu_ref[r, :] = qu.astype(BF16)
        qgt, qut, pdt = qg.T.astype(BF16), qu.T.astype(BF16), pdt_ref[:, r]
        for e in pieces(width, CHUNK):
            update_both(gag0, gag1, nn(qgt, xs_ref[r, e]), block, e)
            update_both(gau0, gau1, nn(qut, xs_ref[r, e]), block, e)
            update_both(gbd0, gbd1, scale * nn(pdt, ds[r, e]), block, e)

    row_blocks(n, rows, start, i == 0)
    row_blocks(n, rows, step)
    row_blocks(n, rows, finish, i == last)

    @pl.when(n <= LO)
    def _():
        for ref in (dg_hi, du_hi):
            ref[...] = jnp.zeros(ref.shape, BF16)

    @pl.when((n <= LO) & (i == last))
    def _():
        for ref in (ds, qg_ref, qu_ref):
            ref[LO:, :] = jnp.zeros((rows - LO, ref.shape[1]), BF16)


def bwd(scale, n, dr, pack, xs, mask, pgt, put, pdt, bd, wd, g, u, bg, bu, ad, tile=1024, depth=3):
    rows, width = dr.shape
    hidden = wd.shape[0]
    half = bd[0].shape[0]
    k = 2 * half
    pair = rows_pair(rows, tile)
    return call(
        functools.partial(bwd_kernel, scale), n, hidden // tile,
        (dr, pack, xs, mask, pgt, put, pdt, *bd, wd, *g, *u, *bg, *bu, *ad),
        [HBM, whole((rows, rows)), whole((rows, width)), whole((rows, k))] + [whole((k, rows))] * 3 + [whole((half, width))] * 2
        + [HBM] + pair * 2 + [col(half, tile)] * 6,
        [Shape((rows, width), BF16)] + [Shape((rows, k), BF16)] * 2 + [Shape((half, width), F32)] * 6
        + pair_shape(rows, hidden, BF16) * 2 + [Shape((half, hidden), F32)] * 6,
        [whole((rows, width))] + [whole((rows, k))] * 2 + [whole((half, width))] * 6 + [col(LO, tile), col(rows - LO, tile)] * 2
        + [col(half, tile)] * 6,
        [pltpu.VMEM((rows, width), BF16), pltpu.VMEM((rows, k), BF16), pltpu.VMEM((k, rows), BF16)]
        + [pltpu.VMEM((rows, k), F32)] * 2 + [pltpu.VMEM((depth, tile, width), BF16)]
        + [pltpu.SemaphoreType.DMA((1, depth)), pltpu.SemaphoreType.DMA],
        1, 2 * width * hidden,
    )


def dx_kernel(
    parts, ds_ref, spread_ref, qg_ref, qu_ref, ag0, ag1, au0, au1, wg_hbm, wu_hbm, dg_lo, dg_hi, du_lo, du_hi,
    back_ref, acc, dgs, dus, sendbuf, wgb, wub, wsem, psem, send_sem, recv_sem, own_sem,
):
    i = pl.program_id(0)
    total = pl.num_programs(0)
    steps = total // parts
    q, t = i // steps, lax.rem(i, steps)
    _, width = ds_ref.shape
    tile = wgb.shape[2]
    part = width // parts
    group, cap = back_ref.shape[:2]
    me = lax.axis_index('data')
    peers = [lax.rem(me + k, group) for k in range(1, group)]
    barrier = pltpu.get_barrier_semaphore()

    @pl.when(i == 0)
    def _():
        for peer in peers:
            pl.semaphore_signal(barrier, inc=1, device_id={'data': peer}, device_id_type=pl.DeviceIdType.MESH)

    def weight(ref):
        def src(s):
            r = pl.multiple_of(s // steps * part, part)
            c = pl.multiple_of(lax.rem(s, steps) * tile, tile)
            return ref.at[pl.ds(r, part), pl.ds(c, tile)]

        return src

    wg, wu = ring(i, total, [(weight(wg_hbm), wgb), (weight(wu_hbm), wub)], wsem)

    def cols(s):
        return pl.ds(pl.multiple_of(s * tile, tile), tile)

    def fills(s):
        pairs = ((dg_lo, dgs, 0), (dg_hi, dgs, LO), (du_lo, dus, 0), (du_hi, dus, LO))
        return [
            pltpu.make_async_copy(src.at[:, cols(s)], dst.at[pl.ds(r, src.shape[0]), cols(s)], psem.at[j, s])
            for j, (src, dst, r) in enumerate(pairs)
        ]

    @pl.when(i == 0)
    def _():
        for s in range(2):
            for copy in fills(s):
                copy.start()

    @pl.when(i + 2 < steps)
    def _():
        for copy in fills(i + 2):
            copy.start()

    @pl.when(i < steps)
    def _():
        for copy in fills(i):
            copy.wait()

    @pl.when(t == 0)
    def _():
        acc[...] = jnp.zeros(acc.shape, F32)

    dg = dgs[:, cols(t)]
    du = dus[:, cols(t)]
    for e in pieces(part, CHUNK // 2):
        acc[:, e] += nt(dg, wg[e, :]) + nt(du, wu[e, :])

    def here(s):
        return pl.ds(pl.multiple_of(s * part, part), part)

    def sends(s):
        return [
            pltpu.make_async_remote_copy(
                src_ref=sendbuf.at[s, peer], dst_ref=back_ref.at[me, :, here(s)], send_sem=send_sem.at[s, peer],
                recv_sem=recv_sem.at[s, me], device_id={'data': peer}, device_id_type=pl.DeviceIdType.MESH,
            )
            for peer in peers
        ]

    def arrivals(s):
        return [
            pltpu.make_async_remote_copy(
                src_ref=sendbuf.at[s, peer], dst_ref=back_ref.at[peer, :, here(s)], send_sem=send_sem.at[s, peer],
                recv_sem=recv_sem.at[s, peer], device_id={'data': peer}, device_id_type=pl.DeviceIdType.MESH,
            )
            for peer in peers
        ]

    def keep(s):
        return pltpu.make_async_copy(sendbuf.at[s, me], back_ref.at[me, :, here(s)], own_sem.at[s])

    @pl.when(t == steps - 1)
    def _():
        c = here(q)
        lora = rounded(nn(qg_ref[...], both(ag0, ag1, c)) + nn(qu_ref[...], both(au0, au1, c)))
        dx = (ds_ref[:, c].astype(F32) + acc[...] + lora).astype(BF16)
        spread = nn(spread_ref[...], dx)
        for p in range(group):
            sendbuf[q, p] = spread[p * cap : (p + 1) * cap].astype(BF16)

        @pl.when(q == 0)
        def _():
            pl.semaphore_wait(barrier, group - 1)

        for copy in sends(q):
            copy.start()
        keep(q).start()

    @pl.when(i == total - 1)
    def _():
        for s in range(parts):
            keep(s).wait()
            for copy in sends(s):
                copy.wait_send()
            for copy in arrivals(s):
                copy.wait_recv()


def dx_all(group, ds, spread, qg, qu, ag, au, wg, wu, dg, du, parts=4, tile=2048, depth=3):
    rows, width = ds.shape
    hidden = wg.shape[1]
    half, k = ag[0].shape[0], qg.shape[1]
    part, cap = width // parts, rows // group
    steps = hidden // tile

    def fixed(shape):
        return pl.BlockSpec(shape, lambda i: (0, 0), pipeline_mode=pl.Buffered(1))

    dma = pltpu.SemaphoreType.DMA
    back = pl.pallas_call(
        functools.partial(dx_kernel, parts),
        grid=(parts * steps,),
        in_specs=[fixed((rows, width)), fixed((rows, rows))] + [fixed((rows, k))] * 2 + [fixed((half, width))] * 4 + [HBM] * 6,
        out_specs=HBM,
        out_shape=Shape((group, cap, width), BF16),
        scratch_shapes=[pltpu.VMEM((rows, part), F32)] + [pltpu.VMEM((rows, hidden), BF16)] * 2 + [pltpu.VMEM((parts, group, cap, part), BF16)]
        + [pltpu.VMEM((depth, part, tile), BF16)] * 2
        + [dma((2, depth)), dma((4, steps)), dma((parts, group)), dma((parts, group)), dma((parts,))],
        compiler_params=pltpu.CompilerParams(
            dimension_semantics=('arbitrary',), vmem_limit_bytes=63_000_000, collective_id=0, has_side_effects=True
        ),
        cost_estimate=pl.CostEstimate(flops=4 * rows * width * hidden, bytes_accessed=4 * width * hidden, transcendentals=0),
    )(ds, spread, qg, qu, *ag, *au, wg, wu, *dg, *du)
    return back.reshape(rows, width)


def solution(mesh):
    group = mesh.shape['data']
    tok = P(('rep', 'data'), None)
    ids_spec = P(('rep', 'data'))
    full = P(None, None)
    own = P('data', None, None)
    grad = P(('rep', 'data'), None, None)
    swap = [(i, i ^ 1) for i in range(group)]

    def layer(x, ids, dy, w_gate, w_up, w_down, a_gate, b_gate, a_up, b_up, a_down, b_down):
        tokens, width = x.shape
        n_local, _, rank = a_gate.shape
        scale = LORA_ALPHA / rank
        cap = ((3 * tokens + 8 * group - 1) // (8 * group)) * 8
        slots = group * cap
        part = cap // 2
        half = n_local * rank
        iota = functools.partial(lax.broadcasted_iota, jnp.int32)

        owner = ids // n_local
        earlier = iota((tokens, tokens), 0) > iota((tokens, tokens), 1)
        order = jnp.sum(jnp.where(earlier & (owner[:, None] == owner[None, :]), 1, 0), axis=1)
        core = (order + owner // 2 + lax.axis_index('data')) % 2
        dest = ((owner // 2) * 2 + core) * cap + (owner % 2) * part + order // 2
        send = (iota((slots, tokens), 0) == dest[None, :]).astype(BF16)
        column = iota((tokens, LANES), 1)
        first = ((owner % 2) ^ core) * half + (ids % n_local) * rank
        flags = ((column >= first[:, None]) & (column < first[:, None] + rank)).astype(BF16)

        def exchange(rows):
            return lax.all_to_all(rows, 'data', 0, 0, tiled=True)

        xr = exchange(nn(send, jnp.concatenate([x, flags], axis=1)).astype(BF16))
        packed_dy, xr = lax.optimization_barrier((nn(send, dy).astype(BF16), xr))
        dr = exchange(packed_dy)

        valid = jnp.sum(xr[:, width:].astype(F32), axis=1) > 0
        upto = (iota((slots, slots), 0) >= iota((slots, slots), 1)) & valid[None, :]
        place = jnp.where(valid, jnp.sum(jnp.where(upto, 1, 0), axis=1) - 1, -1)
        count = jnp.sum(jnp.where(valid, 1, 0)).astype(jnp.int32).reshape(1)
        pack = (place[None, :] == iota((slots, slots), 0)).astype(BF16)
        spread = (place[:, None] == iota((slots, slots), 1)).astype(BF16)

        def flat_a(a):
            v = jnp.swapaxes(a, 1, 2).reshape(half, a.shape[1])
            return v, lax.ppermute(v, 'data', swap)

        def flat_b(b):
            v = b.reshape(half, b.shape[2])
            return v, lax.ppermute(v, 'data', swap)

        ag, au, ad = flat_a(a_gate), flat_a(a_up), flat_a(a_down)
        bg, bu, bd = flat_b(b_gate), flat_b(b_up), flat_b(b_down)

        out_rows, xs, mask, pgt, put, pdt, *gu = fwd(scale, count, xr, pack, spread, ag, au, bd, w_gate, w_up, w_down, bg, bu, ad)
        res = bwd(scale, count, dr, pack, xs, mask, pgt, put, pdt, bd, w_down, gu[:2], gu[2:], bg, bu, ad)
        ds, qg, qu = res[:3]
        dg, du = res[9:11], res[11:13]
        back = [exchange(out_rows)]
        back.append(dx_all(group, ds, spread, qg, qu, ag, au, w_gate, w_up, dg, du))
        sums = [res[j] + lax.ppermute(res[j + 1], 'data', swap) for j in (3, 5, 7, 13, 15, 17)]
        gag, gau, gbd, gbg, gbu, gad = sums

        def shape_a(v):
            return jnp.swapaxes(v.reshape(n_local, rank, v.shape[1]), 1, 2)

        def shape_b(v):
            return v.reshape(n_local, rank, v.shape[1])

        out, dx = [tn(send, v).astype(BF16) for v in back]
        return out, dx, shape_a(gag), shape_b(gbg), shape_a(gau), shape_b(gbu), shape_a(gad), shape_b(gbd)

    return jax.shard_map(
        layer,
        mesh=mesh,
        in_specs=(tok, ids_spec, tok, full, full, full, own, own, own, own, own, own),
        out_specs=(tok, tok, grad, grad, grad, grad, grad, grad),
        check_vma=False,
    )
```

```python
import functools

import jax
import jax.numpy as jnp
from jax import lax
from jax.experimental import pallas as pl
from jax.experimental.pallas import tpu as pltpu
from jax.sharding import PartitionSpec as P


LORA_ALPHA = 32
LANES = 128
CHUNK = 1024
LO = 256
F32 = jnp.float32
BF16 = jnp.bfloat16
Shape = jax.ShapeDtypeStruct
HBM = pl.BlockSpec(memory_space=pl.ANY)


def nn(a, b):
    return lax.dot_general(a, b, (((1,), (0,)), ((), ())), preferred_element_type=F32)


def nt(a, b):
    return lax.dot_general(a, b, (((1,), (1,)), ((), ())), preferred_element_type=F32)


def tn(a, b):
    return lax.dot_general(a, b, (((0,), (0,)), ((), ())), preferred_element_type=F32)


def rounded(v):
    return v.astype(BF16).astype(F32)


def both(a, b, c=slice(None)):
    return jnp.concatenate([a[:, c], b[:, c]], axis=0)


def update_both(a, b, v, block, c=slice(None)):
    half = a.shape[0]
    update(a, c, v[:half], block)
    update(b, c, v[half:], block)


def pieces(width, size):
    return [slice(j, min(j + size, width)) for j in range(0, width, size)]


def row_blocks(n, rows, body, when=None):
    ok = n >= 0 if when is None else when
    pl.when(ok)(functools.partial(body, slice(0, LO), 0))
    pl.when(ok & (n > LO))(functools.partial(body, slice(LO, rows), 1))


def update(ref, c, v, block):
    ref[:, c] = v if block == 0 else ref[:, c] + v


def at_col(ref, tile):
    return lambda t: ref.at[:, pl.ds(pl.multiple_of(t * tile, tile), tile)]


def at_row(ref, tile):
    return lambda t: ref.at[pl.ds(pl.multiple_of(t * tile, tile), tile), :]


def ring(i, steps, items, sems):
    depth = items[0][1].shape[0]

    def copy(t, s, which):
        src, buf = items[which]
        return pltpu.make_async_copy(src(t), buf.at[s], sems.at[which, s])

    @pl.when(i == 0)
    def _():
        for t in range(depth - 1):
            for which in range(len(items)):
                copy(t, t, which).start()

    ahead = i + depth - 1

    @pl.when(ahead < steps)
    def _():
        for which in range(len(items)):
            copy(ahead, lax.rem(ahead, depth), which).start()

    slot = lax.rem(i, depth)
    for which in range(len(items)):
        copy(i, slot, which).wait()
    return [buf.at[slot] for _, buf in items]


def whole(shape):
    return pl.BlockSpec(shape, lambda i, n: (0, 0), pipeline_mode=pl.Buffered(1))


def col(rows, tile):
    return pl.BlockSpec((rows, tile), lambda i, n: (0, i))


def rows_pair(rows, tile):
    upper = pl.BlockSpec((rows - LO, tile), lambda i, n: (0, jnp.where(n[0] > LO, i, 0)))
    return [col(LO, tile), upper]


def pair_shape(rows, width, dtype):
    return [Shape((LO, width), dtype), Shape((rows - LO, width), dtype)]


def call(body, n, steps, args, in_specs, out_shape, out_specs, scratch, products, weight_bytes):
    return pl.pallas_call(
        body,
        grid_spec=pltpu.PrefetchScalarGridSpec(
            num_scalar_prefetch=1, grid=(steps,), in_specs=in_specs, out_specs=out_specs, scratch_shapes=scratch
        ),
        out_shape=out_shape,
        compiler_params=pltpu.CompilerParams(dimension_semantics=('arbitrary',), vmem_limit_bytes=63_000_000),
        cost_estimate=pl.CostEstimate(flops=LO * weight_bytes * products, bytes_accessed=weight_bytes, transcendentals=0),
    )(n, *args)


def fwd_kernel(
    scale, n_ref, xr_ref, pack_ref, spread_ref, ag0, ag1, au0, au1, bd0, bd1, wg_hbm, wu_hbm, wd_hbm, bg0, bg1, bu0, bu1, ad0, ad1,
    out_ref, xs, mask_ref, pgt_ref, put_ref, pdt_ref, g_lo, g_hi, u_lo, u_hi,
    xbuf, oacc, pg_s, pu_s, pd_s, wgb, wub, wdb, wsem, sem,
):
    i = pl.program_id(0)
    last = pl.num_programs(0) - 1
    n = n_ref[0]
    rows, width = xs.shape
    k = pg_s.shape[1]

    @pl.when(i == 0)
    def _():
        pltpu.make_async_copy(xr_ref, xbuf, sem).start()

    tile = wgb.shape[2]
    weights = [(at_col(wg_hbm, tile), wgb), (at_col(wu_hbm, tile), wub), (at_row(wd_hbm, tile), wdb)]
    wg, wu, wd = ring(i, last + 1, weights, wsem)

    @pl.when(i == 0)
    def _():
        pltpu.make_async_copy(xr_ref, xbuf, sem).wait()

    def start(r, block):
        take = pack_ref[r, :]
        for e in pieces(width, CHUNK):
            xs[r, e] = nn(take, xbuf[:, e]).astype(BF16)
        mask_ref[r, :] = nn(take, xbuf[:, width:])[:, :k]
        keep = mask_ref[r, :] > 0
        x = xs[r, :]
        for a, b, s, t in ((ag0, ag1, pg_s, pgt_ref), (au0, au1, pu_s, put_ref)):
            p = jnp.where(keep, nt(x, both(a, b)), 0.0)
            s[r, :] = p.astype(BF16)
            t[:, r] = p.T.astype(BF16)
        oacc[r, :] = jnp.zeros(x.shape, F32)
        pd_s[r, :] = jnp.zeros(keep.shape, F32)

    def step(r, block):
        x = xs[r, :]
        g = nn(x, wg[...]) + rounded(scale * nn(pg_s[r, :], both(bg0, bg1)))
        u = nn(x, wu[...]) + rounded(scale * nn(pu_s[r, :], both(bu0, bu1)))
        (g_lo, g_hi)[block][...] = g
        (u_lo, u_hi)[block][...] = u
        h = (g * jax.nn.sigmoid(g) * u).astype(BF16)
        for e in pieces(width, CHUNK):
            oacc[r, e] += nn(h, wd[:, e])
        pd_s[r, :] += nt(h, both(ad0, ad1))

    def finish(r, block):
        pd = jnp.where(mask_ref[r, :] > 0, pd_s[r, :], 0.0)
        pdt_ref[:, r] = pd.T.astype(BF16)
        pdb = pd.astype(BF16)
        spread = spread_ref[:, r]
        for e in pieces(width, CHUNK):
            out = xs[r, e].astype(F32) + oacc[r, e] + rounded(scale * nn(pdb, both(bd0, bd1, e)))
            update(xbuf, e, nn(spread, out.astype(BF16)).astype(BF16), block)

    row_blocks(n, rows, start, i == 0)
    row_blocks(n, rows, step)
    row_blocks(n, rows, finish, i == last)

    @pl.when(i == last)
    def _():
        save = pltpu.make_async_copy(xbuf.at[:, pl.ds(0, width)], out_ref, sem)
        save.start()
        save.wait()


def fwd(scale, n, xr, pack, spread, ag, au, bd, wg, wu, wd, bg, bu, ad, tile=512, depth=3):
    rows = xr.shape[0]
    width, hidden = wg.shape
    half = ag[0].shape[0]
    k = 2 * half
    return call(
        functools.partial(fwd_kernel, scale), n, hidden // tile,
        (xr, pack, spread, *ag, *au, *bd, wg, wu, wd, *bg, *bu, *ad),
        [HBM] + [whole((rows, rows))] * 2 + [whole((half, width))] * 6 + [HBM] * 3 + [col(half, tile)] * 6,
        [Shape((rows, width), BF16)] * 2 + [Shape((rows, k), F32)] + [Shape((k, rows), BF16)] * 3 + pair_shape(rows, hidden, F32) * 2,
        [HBM, whole((rows, width)), whole((rows, k))] + [whole((k, rows))] * 3 + rows_pair(rows, tile) * 2,
        [pltpu.VMEM(xr.shape, BF16), pltpu.VMEM((rows, width), F32)] + [pltpu.VMEM((rows, k), BF16)] * 2 + [pltpu.VMEM((rows, k), F32)]
        + [pltpu.VMEM((depth, width, tile), BF16)] * 2 + [pltpu.VMEM((depth, tile, width), BF16)]
        + [pltpu.SemaphoreType.DMA((3, depth)), pltpu.SemaphoreType.DMA],
        1, 6 * width * hidden,
    )


def bwd_kernel(
    scale, n_ref, dr_ref, pack_ref, xs_ref, mask_ref, pgt_ref, put_ref, pdt_ref, bd0, bd1,
    wd_hbm, g_lo, g_hi, u_lo, u_hi, bg0, bg1, bu0, bu1, ad0, ad1,
    ds, qg_ref, qu_ref, gag0, gag1, gau0, gau1, gbd0, gbd1, dg_lo, dg_hi, du_lo, du_hi, gbg0, gbg1, gbu0, gbu1, gad0, gad1,
    dbuf, qd_s, qdt_s, qg_s, qu_s, wdb, wsem, sem,
):
    i = pl.program_id(0)
    last = pl.num_programs(0) - 1
    n = n_ref[0]
    rows, width = ds.shape

    @pl.when(i == 0)
    def _():
        pltpu.make_async_copy(dr_ref.at[:, pl.ds(0, width)], dbuf, sem).start()

    wd, = ring(i, last + 1, [(at_row(wd_hbm, wdb.shape[1]), wdb)], wsem)

    @pl.when(i == 0)
    def _():
        pltpu.make_async_copy(dr_ref.at[:, pl.ds(0, width)], dbuf, sem).wait()

    def start(r, block):
        take = pack_ref[r, :]
        for e in pieces(width, CHUNK):
            ds[r, e] = nn(take, dbuf[:, e]).astype(BF16)
        qd = jnp.where(mask_ref[r, :] > 0, scale * nt(ds[r, :], both(bd0, bd1)), 0.0)
        qd_s[r, :] = qd.astype(BF16)
        qdt_s[:, r] = qd.T.astype(BF16)
        for s in (qg_s, qu_s):
            s[r, :] = jnp.zeros(qd.shape, F32)

    def step(r, block):
        for c in pieces(wd.shape[0], CHUNK // 2):
            bg, bu, ad = both(bg0, bg1, c), both(bu0, bu1, c), both(ad0, ad1, c)
            dh = nt(ds[r, :], wd[c, :]) + rounded(nn(qd_s[r, :], ad))
            g = (g_lo, g_hi)[block][:, c]
            u = (u_lo, u_hi)[block][:, c]
            sig = jax.nn.sigmoid(g)
            act = g * sig
            h = (act * u).astype(BF16)
            dg = (dh * u * sig * (1.0 + g * (1.0 - sig))).astype(BF16)
            du = (dh * act).astype(BF16)
            (dg_lo, dg_hi)[block][:, c] = dg
            (du_lo, du_hi)[block][:, c] = du
            qg_s[r, :] += nt(dg, bg)
            qu_s[r, :] += nt(du, bu)
            update_both(gbg0, gbg1, scale * nn(pgt_ref[:, r], dg), block, c)
            update_both(gbu0, gbu1, scale * nn(put_ref[:, r], du), block, c)
            update_both(gad0, gad1, nn(qdt_s[:, r], h), block, c)

    def finish(r, block):
        keep = mask_ref[r, :] > 0
        qg = jnp.where(keep, scale * qg_s[r, :], 0.0)
        qu = jnp.where(keep, scale * qu_s[r, :], 0.0)
        qg_ref[r, :] = qg.astype(BF16)
        qu_ref[r, :] = qu.astype(BF16)
        qgt, qut, pdt = qg.T.astype(BF16), qu.T.astype(BF16), pdt_ref[:, r]
        for e in pieces(width, CHUNK):
            update_both(gag0, gag1, nn(qgt, xs_ref[r, e]), block, e)
            update_both(gau0, gau1, nn(qut, xs_ref[r, e]), block, e)
            update_both(gbd0, gbd1, scale * nn(pdt, ds[r, e]), block, e)

    row_blocks(n, rows, start, i == 0)
    row_blocks(n, rows, step)
    row_blocks(n, rows, finish, i == last)

    @pl.when(n <= LO)
    def _():
        for ref in (dg_hi, du_hi):
            ref[...] = jnp.zeros(ref.shape, BF16)

    @pl.when((n <= LO) & (i == last))
    def _():
        for ref in (ds, qg_ref, qu_ref):
            ref[LO:, :] = jnp.zeros((rows - LO, ref.shape[1]), BF16)


def bwd(scale, n, dr, pack, xs, mask, pgt, put, pdt, bd, wd, g, u, bg, bu, ad, tile=1024, depth=3):
    rows, width = dr.shape[0], wd.shape[1]
    hidden = wd.shape[0]
    half = bd[0].shape[0]
    k = 2 * half
    pair = rows_pair(rows, tile)
    return call(
        functools.partial(bwd_kernel, scale), n, hidden // tile,
        (dr, pack, xs, mask, pgt, put, pdt, *bd, wd, *g, *u, *bg, *bu, *ad),
        [HBM, whole((rows, rows)), whole((rows, width)), whole((rows, k))] + [whole((k, rows))] * 3 + [whole((half, width))] * 2
        + [HBM] + pair * 2 + [col(half, tile)] * 6,
        [Shape((rows, width), BF16)] + [Shape((rows, k), BF16)] * 2 + [Shape((half, width), F32)] * 6
        + pair_shape(rows, hidden, BF16) * 2 + [Shape((half, hidden), F32)] * 6,
        [whole((rows, width))] + [whole((rows, k))] * 2 + [whole((half, width))] * 6 + [col(LO, tile), col(rows - LO, tile)] * 2
        + [col(half, tile)] * 6,
        [pltpu.VMEM((rows, width), BF16), pltpu.VMEM((rows, k), BF16), pltpu.VMEM((k, rows), BF16)]
        + [pltpu.VMEM((rows, k), F32)] * 2 + [pltpu.VMEM((depth, tile, width), BF16)]
        + [pltpu.SemaphoreType.DMA((1, depth)), pltpu.SemaphoreType.DMA],
        1, 2 * width * hidden,
    )


def dx_kernel(
    parts, ds_ref, spread_ref, qg_ref, qu_ref, ag0, ag1, au0, au1, wg_hbm, wu_hbm, dg_lo, dg_hi, du_lo, du_hi,
    back_ref, acc, dgs, dus, sendbuf, wgb, wub, wsem, psem, send_sem, recv_sem, own_sem,
):
    i = pl.program_id(0)
    total = pl.num_programs(0)
    steps = total // parts
    q, t = i // steps, lax.rem(i, steps)
    rows, width = dgs.shape[0], ds_ref.shape[1]
    tile = wgb.shape[2]
    part = width // parts
    group, cap = back_ref.shape[:2]
    me = lax.axis_index('data')
    peers = [lax.rem(me + k, group) for k in range(1, group)]
    barrier = pltpu.get_barrier_semaphore()

    @pl.when(i == 0)
    def _():
        for peer in peers:
            pl.semaphore_signal(barrier, inc=1, device_id={'data': peer}, device_id_type=pl.DeviceIdType.MESH)

    def weight(ref):
        def src(s):
            r = pl.multiple_of(s // steps * part, part)
            c = pl.multiple_of(lax.rem(s, steps) * tile, tile)
            return ref.at[pl.ds(r, part), pl.ds(c, tile)]

        return src

    wg, wu = ring(i, total, [(weight(wg_hbm), wgb), (weight(wu_hbm), wub)], wsem)

    def cols(s):
        return pl.ds(pl.multiple_of(s * tile, tile), tile)

    def fills(s):
        pairs = ((dg_lo, dgs, 0), (du_lo, dus, 0), (dg_hi, dgs, LO), (du_hi, dus, LO))[: 4 if rows > LO else 2]
        return [
            pltpu.make_async_copy(src.at[:, cols(s)], dst.at[pl.ds(r, src.shape[0]), cols(s)], psem.at[j, s])
            for j, (src, dst, r) in enumerate(pairs)
        ]

    @pl.when(i == 0)
    def _():
        for s in range(2):
            for copy in fills(s):
                copy.start()

    @pl.when(i + 2 < steps)
    def _():
        for copy in fills(i + 2):
            copy.start()

    @pl.when(i < steps)
    def _():
        for copy in fills(i):
            copy.wait()

    @pl.when(t == 0)
    def _():
        acc[...] = jnp.zeros(acc.shape, F32)

    def add_rows(r):
        dg = dgs[r, cols(t)]
        du = dus[r, cols(t)]
        for e in pieces(part, CHUNK // 2):
            acc[r, e] += nt(dg, wg[e, :]) + nt(du, wu[e, :])

    def add_block(b, carry):
        add_rows(pl.ds(pl.multiple_of(b * LANES, LANES), LANES))
        return carry

    if rows > LO:
        lax.fori_loop(0, rows // LANES, add_block, 0)
    else:
        add_rows(slice(None))

    def here(s):
        return pl.ds(pl.multiple_of(s * part, part), part)

    def sends(s):
        return [
            pltpu.make_async_remote_copy(
                src_ref=sendbuf.at[s, peer], dst_ref=back_ref.at[me, :, here(s)], send_sem=send_sem.at[s, peer],
                recv_sem=recv_sem.at[s, me], device_id={'data': peer}, device_id_type=pl.DeviceIdType.MESH,
            )
            for peer in peers
        ]

    def arrivals(s):
        return [
            pltpu.make_async_remote_copy(
                src_ref=sendbuf.at[s, peer], dst_ref=back_ref.at[peer, :, here(s)], send_sem=send_sem.at[s, peer],
                recv_sem=recv_sem.at[s, peer], device_id={'data': peer}, device_id_type=pl.DeviceIdType.MESH,
            )
            for peer in peers
        ]

    def keep(s):
        return pltpu.make_async_copy(sendbuf.at[s, me], back_ref.at[me, :, here(s)], own_sem.at[s])

    @pl.when(t == steps - 1)
    def _():
        c = here(q)
        lora = rounded(nn(qg_ref[...], both(ag0, ag1, c)) + nn(qu_ref[...], both(au0, au1, c)))
        dx = (ds_ref[:, c].astype(F32) + acc[...] + lora).astype(BF16)
        spread = nn(spread_ref[:, :rows], dx)
        for p in range(group):
            sendbuf[q, p] = spread[p * cap : (p + 1) * cap].astype(BF16)

        @pl.when(q == 0)
        def _():
            pl.semaphore_wait(barrier, group - 1)

        for copy in sends(q):
            copy.start()
        keep(q).start()

    @pl.when(i == total - 1)
    def _():
        for s in range(parts):
            keep(s).wait()
            for copy in sends(s):
                copy.wait_send()
            for copy in arrivals(s):
                copy.wait_recv()


def dx_all(rows, group, ds, spread, qg, qu, ag, au, wg, wu, dg, du, parts=8, depth=3):
    slots, width = ds.shape
    hidden = wg.shape[1]
    tile = hidden // 4
    half, k = ag[0].shape[0], qg.shape[1]
    part, cap = width // parts, slots // group
    steps = hidden // tile

    def fixed(shape):
        return pl.BlockSpec(shape, lambda i: (0, 0), pipeline_mode=pl.Buffered(1))

    dma = pltpu.SemaphoreType.DMA
    back = pl.pallas_call(
        functools.partial(dx_kernel, parts),
        grid=(parts * steps,),
        in_specs=[fixed((rows, width)), fixed((slots, slots))] + [fixed((rows, k))] * 2 + [fixed((half, width))] * 4 + [HBM] * 6,
        out_specs=HBM,
        out_shape=Shape((group, cap, width), BF16),
        scratch_shapes=[pltpu.VMEM((rows, part), F32)] + [pltpu.VMEM((rows, hidden), BF16)] * 2 + [pltpu.VMEM((parts, group, cap, part), BF16)]
        + [pltpu.VMEM((depth, part, tile), BF16)] * 2
        + [dma((2, depth)), dma((4, steps)), dma((parts, group)), dma((parts, group)), dma((parts,))],
        compiler_params=pltpu.CompilerParams(
            dimension_semantics=('arbitrary',), vmem_limit_bytes=63_000_000, collective_id=rows // LANES, has_side_effects=True
        ),
        cost_estimate=pl.CostEstimate(flops=4 * rows * width * hidden, bytes_accessed=4 * width * hidden, transcendentals=0),
    )(ds, spread, qg, qu, *ag, *au, wg, wu, *dg, *du)
    return back.reshape(slots, width)


def solution(mesh):
    group = mesh.shape['data']
    tok = P(('rep', 'data'), None)
    ids_spec = P(('rep', 'data'))
    full = P(None, None)
    own = P('data', None, None)
    grad = P(('rep', 'data'), None, None)
    swap = [(i, i ^ 1) for i in range(group)]

    def layer(x, ids, dy, w_gate, w_up, w_down, a_gate, b_gate, a_up, b_up, a_down, b_down):
        tokens, width = x.shape
        n_local, _, rank = a_gate.shape
        scale = LORA_ALPHA / rank
        cap = ((3 * tokens + 8 * group - 1) // (8 * group)) * 8
        slots = group * cap
        part = cap // 2
        half = n_local * rank
        iota = functools.partial(lax.broadcasted_iota, jnp.int32)

        owner = ids // n_local
        earlier = iota((tokens, tokens), 0) > iota((tokens, tokens), 1)
        order = jnp.sum(jnp.where(earlier & (owner[:, None] == owner[None, :]), 1, 0), axis=1)
        core = (order + owner // 2 + lax.axis_index('data')) % 2
        dest = ((owner // 2) * 2 + core) * cap + (owner % 2) * part + order // 2
        send = (iota((slots, tokens), 0) == dest[None, :]).astype(BF16)
        column = iota((tokens, LANES), 1)
        first = ((owner % 2) ^ core) * half + (ids % n_local) * rank
        flags = ((column >= first[:, None]) & (column < first[:, None] + rank)).astype(BF16)

        def exchange(rows):
            return lax.all_to_all(rows, 'data', 0, 0, tiled=True)

        xr = exchange(nn(send, jnp.concatenate([x, flags], axis=1)).astype(BF16))
        packed_dy, xr = lax.optimization_barrier((nn(send, jnp.concatenate([dy, flags], axis=1)).astype(BF16), xr))

        valid = jnp.sum(xr[:, width:].astype(F32), axis=1) > 0
        upto = (iota((slots, slots), 0) >= iota((slots, slots), 1)) & valid[None, :]
        place = jnp.where(valid, jnp.sum(jnp.where(upto, 1, 0), axis=1) - 1, -1)
        count = jnp.sum(jnp.where(valid, 1, 0)).astype(jnp.int32).reshape(1)
        full_load = jnp.broadcast_to((count > LO).astype(BF16), (slots, LANES))
        dr = exchange(lax.dynamic_update_slice(packed_dy, full_load, (0, width)))
        any_full = jnp.max(dr[:, width:].astype(F32)) > 0
        pack = (place[None, :] == iota((slots, slots), 0)).astype(BF16)
        spread = (place[:, None] == iota((slots, slots), 1)).astype(BF16)

        def flat_a(a):
            v = jnp.swapaxes(a, 1, 2).reshape(half, a.shape[1])
            return v, lax.ppermute(v, 'data', swap)

        def flat_b(b):
            v = b.reshape(half, b.shape[2])
            return v, lax.ppermute(v, 'data', swap)

        ag, au, ad = flat_a(a_gate), flat_a(a_up), flat_a(a_down)
        bg, bu, bd = flat_b(b_gate), flat_b(b_up), flat_b(b_down)

        out_rows, xs, mask, pgt, put, pdt, *gu = fwd(scale, count, xr, pack, spread, ag, au, bd, w_gate, w_up, w_down, bg, bu, ad)
        res = bwd(scale, count, dr, pack, xs, mask, pgt, put, pdt, bd, w_down, gu[:2], gu[2:], bg, bu, ad)
        ds, qg, qu = res[:3]
        dg, du = res[9:11], res[11:13]
        back = [exchange(out_rows)]
        args = (ds, spread, qg, qu, ag, au, w_gate, w_up, dg, du)
        back.append(lax.cond(any_full, functools.partial(dx_all, slots, group), functools.partial(dx_all, LO, group), *args))
        sums = [res[j] + lax.ppermute(res[j + 1], 'data', swap) for j in (3, 5, 7, 13, 15, 17)]
        gag, gau, gbd, gbg, gbu, gad = sums

        def shape_a(v):
            return jnp.swapaxes(v.reshape(n_local, rank, v.shape[1]), 1, 2)

        def shape_b(v):
            return v.reshape(n_local, rank, v.shape[1])

        out, dx = [tn(send, v).astype(BF16) for v in back]
        return out, dx, shape_a(gag), shape_b(gbg), shape_a(gau), shape_b(gbu), shape_a(gad), shape_b(gbd)

    return jax.shard_map(
        layer,
        mesh=mesh,
        in_specs=(tok, ids_spec, tok, full, full, full, own, own, own, own, own, own),
        out_specs=(tok, tok, grad, grad, grad, grad, grad, grad),
        check_vma=False,
    )
```
